32 devices in a mesh: gx: 4 (over z), gy: 2 (over x), gz: 4 (over y, core).
Axes of the slice: x: 2, y: 2, z: 4, core: 2. Of those that a mesh axis runs over, the one named last changes fastest.
Arguments:
- displacement: float32 [3, 32, 32, 512], P(None, 'gx', 'gy', 'gz'), may hold values from -100 to 100
- density: float32 [32, 32, 512], P('gx', 'gy', 'gz'), may hold values from 0.1 to 1
Outputs:
- aggregate: float32 [], replicated
- adjoint: float32 [3, 32, 32, 512], P(None, 'gx', 'gy', 'gz')
- sensitivity: float32 [32, 32, 512], P('gx', 'gy', 'gz')
The draws below stay inside these ranges and needn't reach their ends.
All inputs are finite; a program needn't handle non-finite values.
Results may differ from the reference program's by a relative error of at most 0.0003.
Values sent between devices are 32-bit elements; how exact they have to be, the bound alone decides.
A program may use at most 64 MiB of HBM per device.

```python
import math
import jax
import jax.numpy as jnp

ITERS = 6
NX = 32
NY = 32
NZ = 512


def face_ramp(length):
    width = max(1, min(16, length // 4))
    position = jnp.arange(length, dtype=jnp.float32)
    distance = jnp.minimum((float(length) - position) / float(width), 1.0)
    return jnp.sin(0.5 * math.pi * distance) ** 2


def draw_displacement(key, part):
    noise_key, sign_key = jax.random.split(jax.random.fold_in(key, 11))
    amplitude = 9.0
    noise = 0.6 * jnp.clip(jax.random.normal(noise_key, (3, NX, NY, NZ), jnp.float32), -6.0, 6.0)
    flip = jnp.where(jax.random.uniform(sign_key, (), jnp.float32) < 0.5, -1.0, 1.0)
    phase = 0.5 * math.pi * jnp.arange(NX, dtype=jnp.float32)
    envelope = face_ramp(NY)[:, None] * face_ramp(NZ)[None, :]
    along = amplitude * flip * jnp.sin(phase)[:, None, None] * envelope[None, :, :]
    across = amplitude * flip * 2.0 / math.sqrt(3.0) * jnp.cos(phase)[:, None, None] * envelope[None, :, :]
    smooth = jnp.stack([along, across, jnp.zeros((NX, NY, NZ), jnp.float32)], axis=0)
    return smooth + noise


def level_of(key, shape, cuts, low, high):
    level, own = 1.0, jax.random.fold_in(key, 6)
    for dim, blocks in cuts:
        steps = jnp.exp(jax.random.uniform(jax.random.fold_in(own, dim), (blocks,), jnp.float32, low / len(cuts), high / len(cuts)))
        level = level * jnp.repeat(steps, shape[dim] // blocks).reshape([-1 if axis == dim else 1 for axis in range(len(shape))])
    return level


def setup_inputs(seed: int = 0) -> dict:
    key_of = jax.random.split(jax.random.key(seed), 3)
    return {
        "displacement": draw_displacement(jax.random.fold_in(key_of[2], 71), 0),
        "density": jnp.clip(0.1 + 0.9 * jax.random.uniform(key_of[1], (NX, NY, NZ), jnp.float32) ** level_of(key_of[1], (NX, NY, NZ), ((0, 4), (1, 2), (2, 4)), -0.2, 0.2), 0.1, 1.0),
    }


lame_first = 0.3 / (1.3 * 0.4)
shear_modulus = 1.0 / 2.6
power_scale = 3.0
damping = 0.6
shift_term = 0.1
diag_factor = (lame_first + 3.0 * shear_modulus) / 16.0
CORNERS = [(first, second, third) for first in (0, 1) for second in (0, 1) for third in (0, 1)]
OFFSETS = [((first, second, third), 2.5 - math.sqrt(first * first + second * second + third * third)) for first in range(-2, 3) for second in range(-2, 3) for third in range(-2, 3) if first * first + second * second + third * third <= 4]

def window(array, anchor, extent):
    return array[:, anchor[0]:anchor[0] + extent[0], anchor[1]:anchor[1] + extent[1], anchor[2]:anchor[2] + extent[2]]

def window_cells(array, anchor, extent):
    return array[anchor[0]:anchor[0] + extent[0], anchor[1]:anchor[1] + extent[1], anchor[2]:anchor[2] + extent[2]]

def gradients(padded, offset, extent):
    totals = [0.0, 0.0, 0.0]
    for corner in CORNERS:
        piece = window(padded, (offset + corner[0], offset + corner[1], offset + corner[2]), extent)
        for direction in range(3):
            totals[direction] = totals[direction] + (2 * corner[direction] - 1) * piece
    return 0.25 * jnp.concatenate(totals, axis=0)

def strains(grad_all):
    return [grad_all[0], grad_all[4], grad_all[8], grad_all[3] + grad_all[1], grad_all[7] + grad_all[5], grad_all[2] + grad_all[6]]

def stiffen(values):
    trace = values[0] + values[1] + values[2]
    return [lame_first * trace + 2.0 * shear_modulus * values[0], lame_first * trace + 2.0 * shear_modulus * values[1], lame_first * trace + 2.0 * shear_modulus * values[2], shear_modulus * values[3], shear_modulus * values[4], shear_modulus * values[5]]

def spread(terms):
    return jnp.stack([terms[0], terms[3], terms[5], terms[3], terms[1], terms[4], terms[5], terms[4], terms[2]], axis=0)

def assemble(padded, extent):
    result = 0.0
    for corner in CORNERS:
        anchor = (1 - corner[0], 1 - corner[1], 1 - corner[2])
        for direction in range(3):
            piece = window(padded[3 * direction:3 * direction + 3], anchor, extent)
            result = result + 0.25 * (2 * corner[direction] - 1) * piece
    return result

def mises(sigma):
    return sigma[0] * sigma[0] + sigma[1] * sigma[1] + sigma[2] * sigma[2] - sigma[0] * sigma[1] - sigma[1] * sigma[2] - sigma[2] * sigma[0] + 3.0 * (sigma[3] * sigma[3] + sigma[4] * sigma[4] + sigma[5] * sigma[5])

def mises_slope(sigma):
    return [2.0 * sigma[0] - sigma[1] - sigma[2], 2.0 * sigma[1] - sigma[2] - sigma[0], 2.0 * sigma[2] - sigma[0] - sigma[1], 6.0 * sigma[3], 6.0 * sigma[4], 6.0 * sigma[5]]

def pad_nodes(field):
    return jnp.pad(field, ((0, 0), (1, 1), (1, 1), (1, 1)))

def reference(displacement, density):
    extent = density.shape
    base = stiffen(strains(gradients(pad_nodes(displacement), 1, extent)))
    rooted = jnp.sqrt(density)
    sigma = [rooted * value for value in base]
    stress = jnp.sqrt(mises(sigma) + 1.0)
    score = power_scale * stress
    top = jnp.max(score)
    total = jnp.sum(jnp.exp(score - top))
    aggregate = (top + jnp.log(total)) / power_scale
    weight = jnp.exp(score - top) / total * float(extent[0] * extent[1] * extent[2])
    factor = weight / (2.0 * stress)
    slope = [factor * value for value in mises_slope(sigma)]
    load = assemble(pad_nodes(spread(stiffen([rooted * value for value in slope]))), extent)
    stiff = 0.01 + 0.99 * density ** 3
    stiff_pad = jnp.pad(stiff, 2)
    summed = 0.0
    for corner in CORNERS:
        summed = summed + window_cells(stiff_pad, (2 - corner[0], 2 - corner[1], 2 - corner[2]), extent)
    diag = diag_factor * summed + shift_term

    def operate(field):
        values = stiffen(strains(gradients(pad_nodes(field), 1, extent)))
        return assemble(pad_nodes(spread([stiff * value for value in values])), extent) + shift_term * field
    adjoint = damping * load / diag
    for sweep in range(1, ITERS):
        adjoint = adjoint + damping * (load - operate(adjoint)) / diag
    other = strains(gradients(pad_nodes(adjoint), 1, extent))
    explicit = sum((slope[index] * base[index] for index in range(6))) / (2.0 * rooted)
    worked = sum((base[index] * other[index] for index in range(6)))
    raw = explicit - 2.97 * density * density * worked
    inside = jnp.pad(jnp.ones(extent, jnp.float32), 2)
    hsum = 0.0
    for offset, factor_w in OFFSETS:
        hsum = hsum + factor_w * window_cells(inside, (2 + offset[0], 2 + offset[1], 2 + offset[2]), extent)
    scaled = jnp.pad(raw / hsum, 2)
    sensitivity = 0.0
    for offset, factor_w in OFFSETS:
        sensitivity = sensitivity + factor_w * window_cells(scaled, (2 + offset[0], 2 + offset[1], 2 + offset[2]), extent)
    return (aggregate, adjoint, sensitivity)
```

```python
import functools
import math

import jax
import jax.numpy as jnp
from jax import lax
from jax.experimental import pallas as pl
from jax.experimental.pallas import tpu as pltpu
from jax.sharding import PartitionSpec as P

ITERS = 6
lame = 0.3 / (1.3 * 0.4)
shear = 1.0 / 2.6
power_scale = 3.0
damping = 0.6
shift_term = 0.1
diag_factor = (lame + 3.0 * shear) / 16.0
FACE = 2.5 - math.sqrt(2.0)
DIAGONAL = 2.5 - math.sqrt(3.0)
MESH = pl.DeviceIdType.MESH
D = 8
C = 16


def gather_kernel(u_ref, rho_ref, out, pack, zs, zr, xs, xr, ys, yr):
    ix, iy, iz = (lax.axis_index(a) for a in ("gx", "gy", "gz"))
    nx, ny, nz = (lax.axis_size(a) for a in ("gx", "gy", "gz"))
    lx, ly, lz = rho_ref.shape
    group = lx + 2
    lane = lax.broadcasted_iota(jnp.int32, (ly, lz), 1)
    for c in range(4):
        first = jnp.zeros((ly, lz), jnp.float32)
        last = first
        for x in range(lx):
            tile = u_ref[c, x] if c < 3 else rho_ref[x]
            out[2 + x, c, 0:ly] = tile
            here = (lane >= C * x) & (lane < C * x + C)
            first = jnp.where(here, pltpu.roll(tile, C * x, 1) if x else tile, first)
            last = jnp.where(here, pltpu.roll(tile, (C * x + C) % lz, 1), last)
        pack[0, c] = first
        pack[1, c] = last

    def send(src, dst, ssem, rsem, axis, target):
        return pltpu.make_async_remote_copy(
            src_ref=src, dst_ref=dst, send_sem=ssem, recv_sem=rsem,
            device_id={axis: target}, device_id_type=MESH)

    def phase(axis, index, count, items):
        for step, src, dst, ssem, rsem in items:
            @pl.when((index + step >= 0) & (index + step < count))
            def _(step=step, src=src, dst=dst, ssem=ssem, rsem=rsem):
                send(src, dst, ssem, rsem, axis, index + step).start()
        for step, src, dst, ssem, rsem in items:
            has = (index - step >= 0) & (index - step < count)

            @pl.when(jnp.logical_not(has))
            def _(dst=dst):
                dst[...] = jnp.zeros(dst.shape, jnp.float32)

            @pl.when(has)
            def _(step=step, src=src, dst=dst, ssem=ssem, rsem=rsem):
                send(src, dst, ssem, rsem, axis, index - step).wait_recv()
        for step, src, dst, ssem, rsem in items:
            @pl.when((index + step >= 0) & (index + step < count))
            def _(step=step, src=src, dst=dst, ssem=ssem, rsem=rsem):
                send(src, dst, ssem, rsem, axis, index + step).wait_send()

    own = pl.ds(0, ly)
    phase("gz", iz, nz, [
        (-1, pack.at[0], out.at[0, :, own], zs.at[0], zr.at[0]),
        (1, pack.at[1], out.at[1, :, own], zs.at[1], zr.at[1]),
    ])
    phase("gx", ix, nx, [
        (1, out.at[pl.ds(0, group), :, own], out.at[pl.ds(group, group), :, own], xs.at[0], xr.at[0]),
        (-1, out.at[pl.ds(0, group), :, own], out.at[pl.ds(2 * group, group), :, own], xs.at[1], xr.at[1]),
        (-2, out.at[pl.ds(0, 3), :, own], out.at[pl.ds(3 * group, 3), :, own], xs.at[2], xr.at[2]),
    ])
    phase("gy", iy, ny, [
        (1, out.at[:, :, pl.ds(ly - D, D)], out.at[:, :, pl.ds(2 * ly, D)], ys.at[0], yr.at[0]),
        (-1, out.at[:, :, pl.ds(0, ly)], out.at[:, :, pl.ds(ly, ly)], ys.at[1], yr.at[1]),
    ])


def up(v, axis):
    return pltpu.roll(v, v.shape[axis] - 1, axis)


def down(v, axis):
    return pltpu.roll(v, 1, axis)


def raw_strain(low, high):
    g = []
    for c in range(3):
        s = low[c] + high[c]
        d = high[c] - low[c]
        s1, d1 = up(s, 1), up(d, 1)
        za, zd, xd = s + s1, s1 - s, d + d1
        g.append((xd + up(xd, 0), up(za, 0) - za, zd + up(zd, 0)))
    return (g[0][0], g[1][1], g[2][2], g[1][0] + g[0][1], g[2][1] + g[1][2], g[0][2] + g[2][0])


def cmul(t):
    tr = lame * (t[0] + t[1] + t[2])
    return [tr + (2.0 * shear) * t[i] for i in range(3)] + [shear * t[i] for i in range(3, 6)]


ROWS = ((0, 3, 5), (3, 1, 4), (5, 4, 2))


def gather_forces(a, b):
    out = []
    for c in range(3):
        i, j, k = ROWS[c]
        x = a[i] - b[i]
        y = a[j] + b[j]
        z = a[k] + b[k]
        w = down(x + y, 0) + (x - y)
        v = down(z, 0) + z
        out.append(down(w + v, 1) + (w - v))
    return out


def compute_kernel(place, ext, adj_out, sens_out, stat, U, RHO, B, VM, JB, S, LOAD, DM, K16, A, Q):
    lx, ly, lz = sens_out.shape
    nx, ny, nz = place[3], place[4], place[5]
    group = lx + 2
    X = lx + 2 * D
    rows, lanes = ly + 2 * D, 2 * lz
    lane = lax.broadcasted_iota(jnp.int32, (2 * ly + D, lz), 1)
    for t in range(X + 1):
        g, xi = divmod(t, lx)
        base = (group, 0, 2 * group, 3 * group)[g]
        for c in range(4):
            if c == 3 and t == X:
                continue
            main = ext[base + 2 + xi, c]
            above = ext[base, c]
            below = ext[base + 1, c]
            if xi:
                above = pltpu.roll(above, lz - C * xi, 1)
            if (lz - C - C * xi) % lz:
                below = pltpu.roll(below, (lz - C - C * xi) % lz, 1)
            if c < 3:
                side = jnp.where(lane < D + 1, above, jnp.where(lane >= lz - D, below, 0.0))
                U[t, c, :, 0:lz] = main
                U[t, c, :, lz:lanes] = side
            else:
                side = jnp.where(lane < D, above, jnp.where(lane >= lz - D, below, 0.0))
                for lo, hi, to in ((0, ly + D, 0), (2 * ly, 2 * ly + D, ly + D)):
                    RHO[t, to:to + hi - lo, 0:lz] = main[lo:hi]
                    RHO[t, to:to + hi - lo, lz:lanes] = side[lo:hi]

    def cut(v):
        return jnp.concatenate([v[0:ly + D], v[2 * ly:2 * ly + D]], axis=0)

    def stage_one(t, best):
        low = [U[t, c] for c in range(3)]
        high = [U[t + 1, c] for c in range(3)]
        b = cmul([cut(0.25 * e) for e in raw_strain(low, high)])
        j = (b[0] * b[0] + b[1] * b[1] + b[2] * b[2] - b[0] * b[1] - b[1] * b[2] - b[2] * b[0]
             + 3.0 * (b[3] * b[3] + b[4] * b[4] + b[5] * b[5]))
        rho = RHO[t]
        vm = jnp.sqrt(rho * j + 1.0)
        for i in range(6):
            B[t, i] = b[i]
        JB[t] = j
        VM[t] = vm
        K16[t] = jnp.where(rho > 0.0, (0.01 + 0.99 * (rho * rho * rho)) * 0.0625, 0.0)
        return jnp.maximum(best, vm)

    best = lax.fori_loop(0, X, stage_one, jnp.ones((rows, lanes), jnp.float32))
    top = power_scale * jnp.max(best)

    def stage_two(t, _):
        vm = VM[t]
        weight = jnp.exp(power_scale * vm - top)
        factor = weight / (2.0 * vm)
        f = factor * RHO[t] * (0.5 * shear)
        b = [B[t, i] for i in range(6)]
        tr = b[0] + b[1] + b[2]
        for i in range(3):
            S[t, i] = f * (3.0 * b[i] - tr)
        for i in range(3, 6):
            S[t, i] = (3.0 * f) * b[i]
        JB[t] = factor * JB[t]
        VM[t] = weight
        return 0

    lax.fori_loop(0, X, stage_two, 0)
    total = jnp.sum(VM[D:D + lx, 0:ly, 0:lz])
    row8 = lax.broadcasted_iota(jnp.int32, stat.shape, 0)
    stat[...] = jnp.where(row8 == 0, top, total)

    def stage_load(t, _):
        f = gather_forces([S[t - 1, i] for i in range(6)], [S[t, i] for i in range(6)])
        k = K16[t - 1] + K16[t]
        k = k + down(k, 0)
        k = k + down(k, 1)
        dm = jnp.where(RHO[t] > 0.0, damping / ((16.0 * diag_factor) * k + shift_term), 0.0)
        DM[t] = dm
        for c in range(3):
            LOAD[t, c] = f[c]
            A[t, c] = dm * f[c]
        return 0

    lax.fori_loop(1, X, stage_load, 0)

    for sweep in range(1, ITERS):
        def stress(t, _):
            k = K16[t]
            v = cmul(raw_strain([A[t, c] for c in range(3)], [A[t + 1, c] for c in range(3)]))
            for i in range(6):
                S[t, i] = k * v[i]
            return 0

        def update(t, _):
            f = gather_forces([S[t - 1, i] for i in range(6)], [S[t, i] for i in range(6)])
            dm = DM[t]
            for c in range(3):
                a = A[t, c]
                A[t, c] = a + dm * (LOAD[t, c] - (f[c] + shift_term * a))
            return 0

        lax.fori_loop(sweep, X - sweep, stress, 0)
        lax.fori_loop(sweep + 1, X - sweep, update, 0)

    for x in range(lx):
        for c in range(3):
            adj_out[c, x] = A[D + x, c, 0:ly, 0:lz]

    y = lax.broadcasted_iota(jnp.int32, (rows, lanes), 0)
    z = lax.broadcasted_iota(jnp.int32, (rows, lanes), 1)
    y = place[1] * ly + jnp.where(y < ly + D, y, y - rows)
    z = place[2] * lz + jnp.where(z < lz + lz // 2, z, z - lanes)
    flat = jnp.where((y >= 0) & (y < ny) & (z >= 0) & (z < nz), 1.0, 0.0)

    def planar(v):
        a1, b1 = up(v, 1), down(v, 1)
        sz = a1 + b1
        sz2 = up(a1, 1) + down(b1, 1)
        vu, vd = up(v, 0), down(v, 0)
        near = sz + (vu + vd)
        far = sz2 + (up(vu, 0) + down(vd, 0))
        corner = up(sz, 0) + down(sz, 0)
        return (2.5 * v + 1.5 * near + FACE * corner + 0.5 * far, 1.5 * v + FACE * near + DIAGONAL * corner, 0.5 * v)

    h0, h1, h2 = planar(flat)

    def inside(i):
        i = place[0] * lx + i
        return jnp.where((i >= 0) & (i < nx), 1.0, 0.0)

    def stage_raw(t, _):
        rho = RHO[t]
        e = raw_strain([A[t, c] for c in range(3)], [A[t + 1, c] for c in range(3)])
        worked = sum(B[t, i] * e[i] for i in range(6))
        raw = JB[t] - (2.97 * 0.25) * (rho * rho) * worked
        i = t - D
        h = h0 * inside(i) + h1 * (inside(i - 1) + inside(i + 1)) + h2 * (inside(i - 2) + inside(i + 2))
        q = planar(jnp.where(rho > 0.0, raw / h, 0.0))
        for j in range(3):
            Q[t - (D - 2), j] = q[j][0:ly, 0:lz]
        return 0

    lax.fori_loop(D - 2, D + lx + 2, stage_raw, 0)
    for x in range(lx):
        sens_out[x] = (Q[x, 2] + Q[x + 1, 1]) + Q[x + 2, 0] + (Q[x + 3, 1] + Q[x + 4, 2])


def on_device(displacement, density):
    lx, ly, lz = density.shape
    axes = ("gx", "gy", "gz")
    counts = [lax.axis_size(a) for a in axes]
    elements = lx * ly * lz * counts[0] * counts[1] * counts[2]
    group = lx + 2
    layers = 3 * group + 3
    vmem = pl.BlockSpec(memory_space=pltpu.VMEM)
    ext = pl.pallas_call(
        gather_kernel,
        out_shape=jax.ShapeDtypeStruct((layers, 4, 2 * ly + D, lz), jnp.float32),
        in_specs=[vmem, vmem],
        out_specs=vmem,
        scratch_shapes=[
            pltpu.VMEM((2, 4, ly, lz), jnp.float32),
            pltpu.SemaphoreType.DMA((2,)),
            pltpu.SemaphoreType.DMA((2,)),
            pltpu.SemaphoreType.DMA((3,)),
            pltpu.SemaphoreType.DMA((3,)),
            pltpu.SemaphoreType.DMA((2,)),
            pltpu.SemaphoreType.DMA((2,)),
        ],
        compiler_params=pltpu.CompilerParams(has_side_effects=True, vmem_limit_bytes=60 * 2**20),
    )(displacement, density)
    place = jnp.stack([lax.axis_index(a) for a in axes]
                      + [jnp.int32(n * s) for n, s in zip(counts, (lx, ly, lz))]).astype(jnp.int32)
    X, R, L = lx + 2 * D, ly + 2 * D, 2 * lz
    f32 = jnp.float32
    adjoint, sens, stat = pl.pallas_call(
        compute_kernel,
        out_shape=(
            jax.ShapeDtypeStruct((3, lx, ly, lz), f32),
            jax.ShapeDtypeStruct((lx, ly, lz), f32),
            jax.ShapeDtypeStruct((2, lz), f32),
        ),
        in_specs=[pl.BlockSpec(memory_space=pltpu.SMEM), vmem],
        out_specs=(vmem, vmem, vmem),
        scratch_shapes=[
            pltpu.VMEM((X + 1, 3, 2 * ly + D, L), f32),
            pltpu.VMEM((X, R, L), f32),
            pltpu.VMEM((X, 6, R, L), f32),
            pltpu.VMEM((X, R, L), f32),
            pltpu.VMEM((X, R, L), f32),
            pltpu.VMEM((X, 6, R, L), f32),
            pltpu.VMEM((X, 3, R, L), f32),
            pltpu.VMEM((X, R, L), f32),
            pltpu.VMEM((X, R, L), f32),
            pltpu.VMEM((X, 3, R, L), f32),
            pltpu.VMEM((lx + 4, 3, ly, lz), f32),
        ],
        compiler_params=pltpu.CompilerParams(vmem_limit_bytes=60 * 2**20),
    )(place, ext)
    tops = lax.all_gather(stat[:, 0], axes)
    top = jnp.max(tops[:, 0])
    total = jnp.sum(tops[:, 1] * jnp.exp(tops[:, 0] - top))
    aggregate = (top + jnp.log(total)) / power_scale
    scale = jnp.exp(stat[0, 0] - top) / total * float(elements)
    return aggregate, adjoint * scale, sens * scale


def solution(mesh):
    return jax.shard_map(
        on_device,
        mesh=mesh,
        in_specs=(P(None, "gx", "gy", "gz"), P("gx", "gy", "gz")),
        out_specs=(P(), P(None, "gx", "gy", "gz"), P("gx", "gy", "gz")),
        check_vma=False,
    )
```

```python
import functools
import math

import jax
import jax.numpy as jnp
from jax import lax
from jax.experimental import pallas as pl
from jax.experimental.pallas import tpu as pltpu
from jax.sharding import PartitionSpec as P

ITERS = 6
lame = 0.3 / (1.3 * 0.4)
shear = 1.0 / 2.6
power_scale = 3.0
damping = 0.6
shift_term = 0.1
diag_factor = (lame + 3.0 * shear) / 16.0
FACE = 2.5 - math.sqrt(2.0)
DIAGONAL = 2.5 - math.sqrt(3.0)
MESH = pl.DeviceIdType.MESH
D = 8
C = 16


class Message:
    def __init__(self, sems, number, axis, step, src, dst, cond=None):
        index, count = lax.axis_index(axis), lax.axis_size(axis)
        self.args = (src, dst, sems[0].at[number], sems[1].at[number], axis, index, step)
        self.sends = (index + step >= 0) & (index + step < count)
        self.gets = (index - step >= 0) & (index - step < count)
        if cond is not None:
            self.sends, self.gets = self.sends & cond, self.gets & cond
        self.dst = dst

    def copy(self, sign):
        src, dst, ssem, rsem, axis, index, step = self.args
        return pltpu.make_async_remote_copy(
            src_ref=src, dst_ref=dst, send_sem=ssem, recv_sem=rsem,
            device_id={axis: index + sign * step}, device_id_type=MESH)

    def start(self):
        pl.when(self.sends)(lambda: self.copy(1).start())

    def clear(self):
        def zero():
            self.dst[...] = jnp.zeros(self.dst.shape, jnp.float32)

        pl.when(jnp.logical_not(self.gets))(zero)

    def arrive(self):
        pl.when(self.gets)(lambda: self.copy(-1).wait_recv())

    def drain(self):
        pl.when(self.sends)(lambda: self.copy(1).wait_send())


def gather(u_ref, rho_ref, ext, T, W, V, pack, ssem, rsem):
    lx, ly, lz = rho_ref.shape
    group = lx + 2
    iy, ny = lax.axis_index("gy"), lax.axis_size("gy")
    has_above, has_below = iy + 1 < ny, iy > 0
    own, upper, lower = pl.ds(0, ly), pl.ds(ly, D), pl.ds(ly + D, D)
    u3, r1, both = pl.ds(0, 3), pl.ds(3, 1), pl.ds(0, 2)
    numbers = iter(range(64))

    def msg(axis, step, src, dst, cond=None):
        return Message((ssem, rsem), next(numbers), axis, step, src, dst, cond)

    def body(g):
        return pl.ds(g * group + 2, lx)

    def whole(g):
        return pl.ds(g * group, group)

    def halo(g):
        return pl.ds(g * group, 2)

    z = [msg("gz", -1, pack.at[0], ext.at[:, 0, own]), msg("gz", 1, pack.at[1], ext.at[:, 1, own])]
    y, x = [], []
    for step, rows, to in ((1, pl.ds(ly - D, D), lower), (-1, pl.ds(0, D), upper)):
        y.append(msg("gy", step, u_ref.at[:, :, rows], ext.at[u3, body(0), to]))
        y.append(msg("gy", step, rho_ref.at[:, rows], ext.at[3, body(0), to]))
    for step, g in ((1, 1), (-1, 2)):
        x.append(msg("gx", step, u_ref, ext.at[u3, body(g), own]))
        x.append(msg("gx", step, rho_ref, ext.at[3, body(g), own]))
    y2, x2, x3 = [], [], []
    for step, rows, to in ((1, pl.ds(ly - D, D), lower), (-1, pl.ds(0, D), upper)):
        y2.append(msg("gy", step, ext.at[:, both, rows], ext.at[:, both, to]))
    y2.append(msg("gy", -1, V, T.at[0]))
    for step, g in ((1, 1), (-1, 2)):
        x2.append(msg("gx", step, ext.at[:, halo(0), own], ext.at[:, halo(g), own]))
        x3.append(msg("gx", step, ext.at[:, whole(0), upper], ext.at[:, whole(g), upper], has_above))
        x3.append(msg("gx", step, ext.at[:, whole(0), lower], ext.at[:, whole(g), lower], has_below))
        x3.append(msg("gx", step, T.at[0], T.at[g], has_above))
    x3.append(msg("gx", -2, T.at[0], T.at[3], has_above))
    x3.append(msg("gx", -2, W.at[0], W.at[1]))
    every = z + y + x + y2 + x2 + x3

    for m in y + x:
        m.start()
    lane = lax.broadcasted_iota(jnp.int32, (ly, lz), 1)
    for c in range(4):
        first = jnp.zeros((ly, lz), jnp.float32)
        last = first
        for i in range(lx):
            tile = u_ref[c, i] if c < 3 else rho_ref[i]
            here = (lane >= C * i) & (lane < C * i + C)
            first = jnp.where(here, pltpu.roll(tile, C * i, 1) if i else tile, first)
            last = jnp.where(here, pltpu.roll(tile, (C * i + C) % lz, 1), last)
        pack[0, c] = first
        pack[1, c] = last
    for m in z:
        m.start()
    for m in every:
        m.clear()
    V[...] = jnp.zeros(V.shape, jnp.float32)
    for c in range(3):
        for i in range(lx):
            k = c * group + 2 + i
            V[k:k + 1] = u_ref[c, i, D:D + 1]
            ext[c, 2 + i, 0:ly] = u_ref[c, i]
    for i in range(lx):
        ext[3, 2 + i, 0:ly] = rho_ref[i]
    for m in z:
        m.arrive()
    for m in x2:
        m.start()
    for m in y2[:2]:
        m.start()
    for c in range(3):
        for i in range(2):
            k = c * group + i
            V[k:k + 1] = ext[c, i, D:D + 1]
    y2[2].start()
    for m in y + y2:
        m.arrive()
    for m in x3[:-1]:
        m.start()
    wide = lax.broadcasted_iota(jnp.int32, (ly + 2 * D, lz), 1)
    side = jnp.zeros((ly + 2 * D, lz), jnp.float32)
    for c in range(3):
        W[0, c] = ext[c, 2]
        for i in range(2):
            at = 2 * C * c + C * i
            tile = ext[c, i]
            tile = pltpu.roll(tile, at, 1) if at else tile
            side = jnp.where((wide >= at) & (wide < at + C), tile, side)
    W[0, 3] = side
    x3[-1].start()
    for m in x + x2 + x3:
        m.arrive()
    return every


def up(v, axis):
    return pltpu.roll(v, v.shape[axis] - 1, axis)


def down(v, axis):
    return pltpu.roll(v, 1, axis)


def raw_strain(low, high):
    g = []
    for c in range(3):
        s = low[c] + high[c]
        d = high[c] - low[c]
        s1, d1 = up(s, 1), up(d, 1)
        za, zd, xd = s + s1, s1 - s, d + d1
        g.append((xd + up(xd, 0), up(za, 0) - za, zd + up(zd, 0)))
    return (g[0][0], g[1][1], g[2][2], g[1][0] + g[0][1], g[2][1] + g[1][2], g[0][2] + g[2][0])


def cmul(t):
    tr = lame * (t[0] + t[1] + t[2])
    return [tr + (2.0 * shear) * t[i] for i in range(3)] + [shear * t[i] for i in range(3, 6)]


ROWS = ((0, 3, 5), (3, 1, 4), (5, 4, 2))


def gather_forces(a, b):
    out = []
    for c in range(3):
        i, j, k = ROWS[c]
        x = a[i] - b[i]
        y = a[j] + b[j]
        z = a[k] + b[k]
        w = down(x + y, 0) + (x - y)
        v = down(z, 0) + z
        out.append(down(w + v, 1) + (w - v))
    return out


def kernel(u_ref, rho_ref, agg_out, adj_out, sens_out, ext, T, W, V, pack, ssem, rsem, ST, gsem, hsem, U, RHO, B, VM, JB, S, LOAD, DM, K16, A, Q):
    lx, ly, lz = sens_out.shape
    axes = ("gx", "gy", "gz")
    place = [lax.axis_index(a) for a in axes]
    counts = [lax.axis_size(a) for a in axes]
    nx, ny, nz = counts[0] * lx, counts[1] * ly, counts[2] * lz
    devices = counts[0] * counts[1] * counts[2]
    me = (place[0] * counts[1] + place[1]) * counts[2] + place[2]
    group = lx + 2
    pending = gather(u_ref, rho_ref, ext, T, W, V, pack, ssem, rsem)
    X = lx + 2 * D
    rows, lanes = ly + 2 * D, 2 * lz
    wide = (ly + 3 * D, lz)
    lane = lax.broadcasted_iota(jnp.int32, wide, 1)

    def tall(v, row):
        return jnp.concatenate([v[0:ly + D], jnp.broadcast_to(row, (D, lz)), v[ly + D:rows]], axis=0)

    def turn(v, amount):
        return pltpu.roll(v, amount % lz, 1) if amount % lz else v

    for t in range(X + 1):
        g, xi = divmod(t, lx)
        base = (group, 0, 2 * group, 0)[g]
        tg = (1, 0, 2, 3)[g]
        for c in range(3):
            k = c * group
            if t < X:
                main, above, below = ext[c, base + 2 + xi], ext[c, base], ext[c, base + 1]
                above, below = turn(above, -C * xi), turn(below, -C - C * xi)
            else:
                main, side = W[1, c], W[1, 3]
                above, below = turn(side, -2 * C * c), turn(side, -2 * C * c - 2 * C)
            above = tall(above, turn(T[tg, k:k + 1], -C * xi))
            below = tall(below, turn(T[tg, k + 1:k + 2], -C - C * xi))
            U[t, c, :, 0:lz] = tall(main, T[tg, k + 2 + xi:k + 3 + xi])
            U[t, c, :, lz:lanes] = jnp.where(lane < D + 1, above, jnp.where(lane >= lz - D, below, 0.0))
        if t < X:
            above, below = turn(ext[3, base], -C * xi), turn(ext[3, base + 1], -C - C * xi)
            thin = lane[0:rows]
            RHO[t, :, 0:lz] = ext[3, base + 2 + xi]
            RHO[t, :, lz:lanes] = jnp.where(thin < D, above, jnp.where(thin >= lz - D, below, 0.0))

    def cut(v):
        return jnp.concatenate([v[0:ly + D], v[ly + 2 * D:ly + 3 * D]], axis=0)

    def stage_one(t, best):
        low = [U[t, c] for c in range(3)]
        high = [U[t + 1, c] for c in range(3)]
        b = cmul([cut(0.25 * e) for e in raw_strain(low, high)])
        j = (b[0] * b[0] + b[1] * b[1] + b[2] * b[2] - b[0] * b[1] - b[1] * b[2] - b[2] * b[0]
             + 3.0 * (b[3] * b[3] + b[4] * b[4] + b[5] * b[5]))
        rho = RHO[t]
        vm = jnp.sqrt(rho * j + 1.0)
        for i in range(6):
            B[t, i] = b[i]
        JB[t] = j
        VM[t] = vm
        K16[t] = jnp.where(rho > 0.0, (0.01 + 0.99 * (rho * rho * rho)) * 0.0625, 0.0)
        return jnp.maximum(best, vm)

    best = lax.fori_loop(0, X, stage_one, jnp.ones((rows, lanes), jnp.float32))
    top = power_scale * jnp.max(best)

    def stage_two(t, _):
        vm = VM[t]
        weight = jnp.exp(power_scale * vm - top)
        factor = weight / (2.0 * vm)
        f = factor * RHO[t] * (0.5 * shear)
        b = [B[t, i] for i in range(6)]
        tr = b[0] + b[1] + b[2]
        for i in range(3):
            S[t, i] = f * (3.0 * b[i] - tr)
        for i in range(3, 6):
            S[t, i] = (3.0 * f) * b[i]
        JB[t] = factor * JB[t]
        VM[t] = weight
        return 0

    lax.fori_loop(0, X, stage_two, 0)
    total = jnp.sum(VM[D:D + lx, 0:ly, 0:lz])
    row8 = lax.broadcasted_iota(jnp.int32, (8, lz), 0)
    ST[me] = jnp.where(row8 == 0, top, total)

    def partner(k, sign):
        other = (me + sign * k + devices) % devices
        there = (other // (counts[1] * counts[2]), (other // counts[2]) % counts[1], other % counts[2])
        slot = me if sign > 0 else other
        return pltpu.make_async_remote_copy(
            src_ref=ST.at[slot], dst_ref=ST.at[slot], send_sem=gsem.at[k], recv_sem=hsem.at[k],
            device_id=there, device_id_type=MESH)

    def give(k, _):
        partner(k, 1).start()
        return 0

    lax.fori_loop(1, devices, give, 0)

    def stage_load(t, _):
        f = gather_forces([S[t - 1, i] for i in range(6)], [S[t, i] for i in range(6)])
        k = K16[t - 1] + K16[t]
        k = k + down(k, 0)
        k = k + down(k, 1)
        dm = jnp.where(RHO[t] > 0.0, damping / ((16.0 * diag_factor) * k + shift_term), 0.0)
        DM[t] = dm
        for c in range(3):
            LOAD[t, c] = f[c]
            A[t, c] = dm * f[c]
        return 0

    lax.fori_loop(1, X, stage_load, 0)

    for sweep in range(1, ITERS):
        def stress(t, _):
            k = K16[t]
            v = cmul(raw_strain([A[t, c] for c in range(3)], [A[t + 1, c] for c in range(3)]))
            for i in range(6):
                S[t, i] = k * v[i]
            return 0

        def update(t, _):
            f = gather_forces([S[t - 1, i] for i in range(6)], [S[t, i] for i in range(6)])
            dm = DM[t]
            for c in range(3):
                a = A[t, c]
                A[t, c] = a + dm * (LOAD[t, c] - (f[c] + shift_term * a))
            return 0

        lax.fori_loop(sweep, X - sweep, stress, 0)
        lax.fori_loop(sweep + 1, X - sweep, update, 0)

    y = lax.broadcasted_iota(jnp.int32, (rows, lanes), 0)
    z = lax.broadcasted_iota(jnp.int32, (rows, lanes), 1)
    y = place[1] * ly + jnp.where(y < ly + D, y, y - rows)
    z = place[2] * lz + jnp.where(z < lz + lz // 2, z, z - lanes)
    flat = jnp.where((y >= 0) & (y < ny) & (z >= 0) & (z < nz), 1.0, 0.0)

    def planar(v):
        a1, b1 = up(v, 1), down(v, 1)
        sz = a1 + b1
        sz2 = up(a1, 1) + down(b1, 1)
        vu, vd = up(v, 0), down(v, 0)
        near = sz + (vu + vd)
        far = sz2 + (up(vu, 0) + down(vd, 0))
        corner = up(sz, 0) + down(sz, 0)
        return (2.5 * v + 1.5 * near + FACE * corner + 0.5 * far, 1.5 * v + FACE * near + DIAGONAL * corner, 0.5 * v)

    h0, h1, h2 = planar(flat)

    def inside(i):
        i = place[0] * lx + i
        return jnp.where((i >= 0) & (i < nx), 1.0, 0.0)

    def stage_raw(t, _):
        rho = RHO[t]
        e = raw_strain([A[t, c] for c in range(3)], [A[t + 1, c] for c in range(3)])
        worked = sum(B[t, i] * e[i] for i in range(6))
        raw = JB[t] - (2.97 * 0.25) * (rho * rho) * worked
        i = t - D
        h = h0 * inside(i) + h1 * (inside(i - 1) + inside(i + 1)) + h2 * (inside(i - 2) + inside(i + 2))
        q = planar(jnp.where(rho > 0.0, raw / h, 0.0))
        for j in range(3):
            Q[t - (D - 2), j] = q[j][0:ly, 0:lz]
        return 0

    lax.fori_loop(D - 2, D + lx + 2, stage_raw, 0)

    def take(k, _):
        partner(k, -1).wait_recv()
        partner(k, 1).wait_send()
        return 0

    lax.fori_loop(1, devices, take, 0)
    for m in pending:
        m.drain()
    tops, totals = ST[:, 0, :], ST[:, 1, :]
    peak = jnp.max(tops, axis=0, keepdims=True)
    sums = jnp.sum(totals * jnp.exp(tops - peak), axis=0, keepdims=True)
    agg_out[0, 0] = jnp.max((peak + jnp.log(sums)) / power_scale)
    scale = jnp.exp(top - peak) / sums * float(nx * ny * nz)
    for x in range(lx):
        for c in range(3):
            adj_out[c, x] = A[D + x, c, 0:ly, 0:lz] * scale
        sens_out[x] = ((Q[x, 2] + Q[x + 1, 1]) + Q[x + 2, 0] + (Q[x + 3, 1] + Q[x + 4, 2])) * scale


def on_device(displacement, density):
    lx, ly, lz = density.shape
    devices = lax.axis_size("gx") * lax.axis_size("gy") * lax.axis_size("gz")
    group = lx + 2
    vmem = pl.BlockSpec(memory_space=pltpu.VMEM)
    X, R, L = lx + 2 * D, ly + 2 * D, 2 * lz
    f32 = jnp.float32
    shapes = [
        (X + 1, 3, ly + 3 * D, L), (X, R, L), (X, 6, R, L), (X, R, L), (X, R, L), (X, 6, R, L),
        (X, 3, R, L), (X, R, L), (X, R, L), (X, 3, R, L), (lx + 4, 3, ly, lz),
    ]
    dma = pltpu.SemaphoreType.DMA
    aggregate, adjoint, sens = pl.pallas_call(
        kernel,
        out_shape=(
            jax.ShapeDtypeStruct((1, 1), f32),
            jax.ShapeDtypeStruct((3, lx, ly, lz), f32),
            jax.ShapeDtypeStruct((lx, ly, lz), f32),
        ),
        in_specs=[vmem, vmem],
        out_specs=(pl.BlockSpec(memory_space=pltpu.SMEM), vmem, vmem),
        scratch_shapes=[
            pltpu.VMEM((4, 3 * group, R, lz), f32),
            pltpu.VMEM((4, 32, lz), f32),
            pltpu.VMEM((2, 4, R, lz), f32),
            pltpu.VMEM((32, lz), f32),
            pltpu.VMEM((2, 4, ly, lz), f32),
            dma((32,)), dma((32,)),
            pltpu.VMEM((devices, 8, lz), f32),
            dma((devices,)), dma((devices,)),
        ] + [pltpu.VMEM(s, f32) for s in shapes],
        compiler_params=pltpu.CompilerParams(has_side_effects=True, vmem_limit_bytes=60 * 2**20),
    )(displacement, density)
    return aggregate[0, 0], adjoint, sens


def solution(mesh):
    return jax.shard_map(
        on_device,
        mesh=mesh,
        in_specs=(P(None, "gx", "gy", "gz"), P("gx", "gy", "gz")),
        out_specs=(P(), P(None, "gx", "gy", "gz"), P("gx", "gy", "gz")),
        check_vma=False,
    )
```

```python
import functools
import math

import jax
import jax.numpy as jnp
from jax import lax
from jax.experimental import pallas as pl
from jax.experimental.pallas import tpu as pltpu
from jax.sharding import PartitionSpec as P

ITERS = 6
lame = 0.3 / (1.3 * 0.4)
shear = 1.0 / 2.6
power_scale = 3.0
damping = 0.6
shift_term = 0.1
diag_factor = (lame + 3.0 * shear) / 16.0
FACE = 2.5 - math.sqrt(2.0)
DIAGONAL = 2.5 - math.sqrt(3.0)
MESH = pl.DeviceIdType.MESH
D = 8
C = 16


class Message:
    def __init__(self, sems, number, axis, step, src, dst, cond=None):
        index, count = lax.axis_index(axis), lax.axis_size(axis)
        self.args = (src, dst, sems[0].at[number], sems[1].at[number], axis, index, step)
        self.sends = (index + step >= 0) & (index + step < count)
        self.gets = (index - step >= 0) & (index - step < count)
        if cond is not None:
            self.sends, self.gets = self.sends & cond, self.gets & cond
        self.dst = dst

    def copy(self, sign):
        src, dst, ssem, rsem, axis, index, step = self.args
        return pltpu.make_async_remote_copy(
            src_ref=src, dst_ref=dst, send_sem=ssem, recv_sem=rsem,
            device_id={axis: index + sign * step}, device_id_type=MESH)

    def start(self):
        pl.when(self.sends)(lambda: self.copy(1).start())

    def clear(self):
        def zero():
            self.dst[...] = jnp.zeros(self.dst.shape, jnp.float32)

        pl.when(jnp.logical_not(self.gets))(zero)

    def arrive(self):
        pl.when(self.gets)(lambda: self.copy(-1).wait_recv())

    def drain(self):
        pl.when(self.sends)(lambda: self.copy(1).wait_send())


def gather(u_ref, rho_ref, ext, T, W, V, pack, ssem, rsem):
    lx, ly, lz = rho_ref.shape
    group = lx + 2
    iy, ny = lax.axis_index("gy"), lax.axis_size("gy")
    has_above, has_below = iy + 1 < ny, iy > 0
    own, upper, lower = pl.ds(0, ly), pl.ds(ly, D), pl.ds(ly + D, D)
    u3, r1, both = pl.ds(0, 3), pl.ds(3, 1), pl.ds(0, 2)
    numbers = iter(range(64))

    def msg(axis, step, src, dst, cond=None):
        return Message((ssem, rsem), next(numbers), axis, step, src, dst, cond)

    def body(g):
        return pl.ds(g * group + 2, lx)

    def whole(g):
        return pl.ds(g * group, group)

    def halo(g):
        return pl.ds(g * group, 2)

    z = [msg("gz", -1, pack.at[0], ext.at[:, 0, own]), msg("gz", 1, pack.at[1], ext.at[:, 1, own])]
    y, x = [], []
    for step, rows, to in ((1, pl.ds(ly - D, D), lower), (-1, pl.ds(0, D), upper)):
        y.append(msg("gy", step, u_ref.at[:, :, rows], ext.at[u3, body(0), to]))
        y.append(msg("gy", step, rho_ref.at[:, rows], ext.at[3, body(0), to]))
    for step, g in ((1, 1), (-1, 2)):
        x.append(msg("gx", step, u_ref, ext.at[u3, body(g), own]))
        x.append(msg("gx", step, rho_ref, ext.at[3, body(g), own]))
    y2, x2, x3 = [], [], []
    for step, rows, to in ((1, pl.ds(ly - D, D), lower), (-1, pl.ds(0, D), upper)):
        y2.append(msg("gy", step, ext.at[:, both, rows], ext.at[:, both, to]))
    y2.append(msg("gy", -1, V, T.at[0]))
    for step, g in ((1, 1), (-1, 2)):
        x2.append(msg("gx", step, ext.at[:, halo(0), own], ext.at[:, halo(g), own]))
        x3.append(msg("gx", step, ext.at[:, whole(0), upper], ext.at[:, whole(g), upper], has_above))
        x3.append(msg("gx", step, ext.at[:, whole(0), lower], ext.at[:, whole(g), lower], has_below))
        x3.append(msg("gx", step, T.at[0], T.at[g], has_above))
    x3.append(msg("gx", -2, T.at[0], T.at[3], has_above))
    x3.append(msg("gx", -2, W.at[0], W.at[1]))
    every = z + y + x + y2 + x2 + x3

    for m in y + x:
        m.start()
    lane = lax.broadcasted_iota(jnp.int32, (ly, lz), 1)
    for c in range(4):
        first = jnp.zeros((ly, lz), jnp.float32)
        last = first
        for i in range(lx):
            tile = u_ref[c, i] if c < 3 else rho_ref[i]
            here = (lane >= C * i) & (lane < C * i + C)
            first = jnp.where(here, pltpu.roll(tile, C * i, 1) if i else tile, first)
            last = jnp.where(here, pltpu.roll(tile, (C * i + C) % lz, 1), last)
        pack[0, c] = first
        pack[1, c] = last
    for m in z:
        m.start()
    for m in every:
        m.clear()
    V[...] = jnp.zeros(V.shape, jnp.float32)
    for c in range(3):
        for i in range(lx):
            k = c * group + 2 + i
            V[k:k + 1] = u_ref[c, i, D:D + 1]
            ext[c, 2 + i, 0:ly] = u_ref[c, i]
    for i in range(lx):
        ext[3, 2 + i, 0:ly] = rho_ref[i]
    for m in z:
        m.arrive()
    for m in x2:
        m.start()
    for m in y2[:2]:
        m.start()
    for c in range(3):
        for i in range(2):
            k = c * group + i
            V[k:k + 1] = ext[c, i, D:D + 1]
    y2[2].start()
    for m in y + y2:
        m.arrive()
    for m in x3[:-1]:
        m.start()
    wide = lax.broadcasted_iota(jnp.int32, (ly + 2 * D, lz), 1)
    side = jnp.zeros((ly + 2 * D, lz), jnp.float32)
    for c in range(3):
        W[0, c] = ext[c, 2]
        for i in range(2):
            at = 2 * C * c + C * i
            tile = ext[c, i]
            tile = pltpu.roll(tile, at, 1) if at else tile
            side = jnp.where((wide >= at) & (wide < at + C), tile, side)
    W[0, 3] = side
    x3[-1].start()
    lower_side = x[:2] + x2[:1] + x3[:3]
    upper_side = x[2:] + x2[1:] + x3[3:6]
    return every, (lower_side, upper_side, x3[6:])


def up(v, axis):
    return pltpu.roll(v, v.shape[axis] - 1, axis)


def down(v, axis):
    return pltpu.roll(v, 1, axis)


def raw_strain(low, high):
    g = []
    for c in range(3):
        s = low[c] + high[c]
        d = high[c] - low[c]
        s1, d1 = up(s, 1), up(d, 1)
        za, zd, xd = s + s1, s1 - s, d + d1
        g.append((xd + up(xd, 0), up(za, 0) - za, zd + up(zd, 0)))
    return (g[0][0], g[1][1], g[2][2], g[1][0] + g[0][1], g[2][1] + g[1][2], g[0][2] + g[2][0])


def cmul(t):
    tr = lame * (t[0] + t[1] + t[2])
    return [tr + (2.0 * shear) * t[i] for i in range(3)] + [shear * t[i] for i in range(3, 6)]


ROWS = ((0, 3, 5), (3, 1, 4), (5, 4, 2))


def gather_forces(a, b):
    out = []
    for c in range(3):
        i, j, k = ROWS[c]
        x = a[i] - b[i]
        y = a[j] + b[j]
        z = a[k] + b[k]
        w = down(x + y, 0) + (x - y)
        v = down(z, 0) + z
        out.append(down(w + v, 1) + (w - v))
    return out


def kernel(u_ref, rho_ref, agg_out, adj_out, sens_out, ext, T, W, V, pack, ssem, rsem, ST, gsem, hsem, U, RHO, B, VM, JB, S, LOAD, DM, K16, A, Q):
    lx, ly, lz = sens_out.shape
    axes = ("gx", "gy", "gz")
    barrier = pltpu.get_barrier_semaphore()
    friends = 0
    for axis in axes:
        index, count = lax.axis_index(axis), lax.axis_size(axis)
        friends += count - 1
        for step in range(1, count):
            pl.semaphore_signal(barrier, inc=1, device_id={axis: (index + step) % count}, device_id_type=MESH)
    pl.semaphore_wait(barrier, friends)
    place = [lax.axis_index(a) for a in axes]
    counts = [lax.axis_size(a) for a in axes]
    nx, ny, nz = counts[0] * lx, counts[1] * ly, counts[2] * lz
    group = lx + 2
    pending, arrivals = gather(u_ref, rho_ref, ext, T, W, V, pack, ssem, rsem)
    X = lx + 2 * D
    rows, lanes = ly + 2 * D, 2 * lz
    wide = (ly + 3 * D, lz)
    lane = lax.broadcasted_iota(jnp.int32, wide, 1)

    def tall(v, row):
        return jnp.concatenate([v[0:ly + D], jnp.broadcast_to(row, (D, lz)), v[ly + D:rows]], axis=0)

    def turn(v, amount):
        return pltpu.roll(v, amount % lz, 1) if amount % lz else v

    def unpack(t):
        g, xi = divmod(t, lx)
        base = (group, 0, 2 * group, 0)[g]
        tg = (1, 0, 2, 3)[g]
        for c in range(3):
            k = c * group
            if t < X:
                main, above, below = ext[c, base + 2 + xi], ext[c, base], ext[c, base + 1]
                above, below = turn(above, -C * xi), turn(below, -C - C * xi)
            else:
                main, side = W[1, c], W[1, 3]
                above, below = turn(side, -2 * C * c), turn(side, -2 * C * c - 2 * C)
            above = tall(above, turn(T[tg, k:k + 1], -C * xi))
            below = tall(below, turn(T[tg, k + 1:k + 2], -C - C * xi))
            U[t, c, :, 0:lz] = tall(main, T[tg, k + 2 + xi:k + 3 + xi])
            U[t, c, :, lz:lanes] = jnp.where(lane < D + 1, above, jnp.where(lane >= lz - D, below, 0.0))
        if t < X:
            above, below = turn(ext[3, base], -C * xi), turn(ext[3, base + 1], -C - C * xi)
            thin = lane[0:rows]
            RHO[t, :, 0:lz] = ext[3, base + 2 + xi]
            RHO[t, :, lz:lanes] = jnp.where(thin < D, above, jnp.where(thin >= lz - D, below, 0.0))

    def cut(v):
        return jnp.concatenate([v[0:ly + D], v[ly + 2 * D:ly + 3 * D]], axis=0)

    def stage_one(t, best):
        low = [U[t, c] for c in range(3)]
        high = [U[t + 1, c] for c in range(3)]
        b = cmul([cut(0.25 * e) for e in raw_strain(low, high)])
        j = (b[0] * b[0] + b[1] * b[1] + b[2] * b[2] - b[0] * b[1] - b[1] * b[2] - b[2] * b[0]
             + 3.0 * (b[3] * b[3] + b[4] * b[4] + b[5] * b[5]))
        rho = RHO[t]
        vm = jnp.sqrt(rho * j + 1.0)
        for i in range(6):
            B[t, i] = b[i]
        JB[t] = j
        VM[t] = vm
        K16[t] = jnp.where(rho > 0.0, (0.01 + 0.99 * (rho * rho * rho)) * 0.0625, 0.0)
        return jnp.maximum(best, vm)

    best = jnp.ones((rows, lanes), jnp.float32)
    for t in range(D, D + lx):
        unpack(t)
    best = lax.fori_loop(D, D + lx - 1, stage_one, best)
    for m in arrivals[0]:
        m.arrive()
    for t in range(D):
        unpack(t)
    best = lax.fori_loop(0, D, stage_one, best)
    for m in arrivals[1]:
        m.arrive()
    for t in range(D + lx, X):
        unpack(t)
    best = lax.fori_loop(D + lx - 1, X - 1, stage_one, best)
    for m in arrivals[2]:
        m.arrive()
    unpack(X)
    best = stage_one(X - 1, best)
    top = power_scale * jnp.max(best)

    def stage_two(t, _):
        vm = VM[t]
        weight = jnp.exp(power_scale * vm - top)
        factor = weight / (2.0 * vm)
        f = factor * RHO[t] * (0.5 * shear)
        b = [B[t, i] for i in range(6)]
        tr = b[0] + b[1] + b[2]
        for i in range(3):
            S[t, i] = f * (3.0 * b[i] - tr)
        for i in range(3, 6):
            S[t, i] = (3.0 * f) * b[i]
        JB[t] = factor * JB[t]
        VM[t] = weight
        return 0

    lax.fori_loop(0, X, stage_two, 0)
    total = jnp.sum(VM[D:D + lx, 0:ly, 0:lz])
    row8 = lax.broadcasted_iota(jnp.int32, (8, lz), 0)
    starts = (0, counts[0], counts[0] + counts[1])
    state = jnp.where(row8 == 0, top, total)

    def partner(p, k, sign):
        index, count = place[p], counts[p]
        other = (index + sign * k) % count if sign > 0 else (index - k + count) % count
        slot = starts[p] + (index if sign > 0 else other)
        return pltpu.make_async_remote_copy(
            src_ref=ST.at[slot], dst_ref=ST.at[slot],
            send_sem=gsem.at[starts[p] + k], recv_sem=hsem.at[starts[p] + k],
            device_id={axes[p]: other}, device_id_type=MESH)

    def give(p, value):
        ST[starts[p] + place[p]] = value
        for k in range(1, counts[p]):
            partner(p, k, 1).start()

    def take(p):
        for k in range(1, counts[p]):
            partner(p, k, -1).wait_recv()
        for k in range(1, counts[p]):
            partner(p, k, 1).wait_send()
        tiles = ST[starts[p]:starts[p] + counts[p]]
        tops, totals = tiles[:, 0, :], tiles[:, 1, :]
        peak = jnp.max(tops, axis=0, keepdims=True)
        sums = jnp.sum(totals * jnp.exp(tops - peak), axis=0, keepdims=True)
        return peak, sums

    give(0, state)

    def stage_load(t, _):
        f = gather_forces([S[t - 1, i] for i in range(6)], [S[t, i] for i in range(6)])
        k = K16[t - 1] + K16[t]
        k = k + down(k, 0)
        k = k + down(k, 1)
        dm = jnp.where(RHO[t] > 0.0, damping / ((16.0 * diag_factor) * k + shift_term), 0.0)
        DM[t] = dm
        for c in range(3):
            LOAD[t, c] = f[c]
            A[t, c] = dm * f[c]
        return 0

    lax.fori_loop(1, X, stage_load, 0)

    for sweep in range(1, ITERS):
        def stress(t, _):
            k = K16[t]
            v = cmul(raw_strain([A[t, c] for c in range(3)], [A[t + 1, c] for c in range(3)]))
            for i in range(6):
                S[t, i] = k * v[i]
            return 0

        def update(t, _):
            f = gather_forces([S[t - 1, i] for i in range(6)], [S[t, i] for i in range(6)])
            dm = DM[t]
            for c in range(3):
                a = A[t, c]
                A[t, c] = a + dm * (LOAD[t, c] - (f[c] + shift_term * a))
            return 0

        lax.fori_loop(sweep, X - sweep, stress, 0)
        lax.fori_loop(sweep + 1, X - sweep, update, 0)
        if sweep <= 2:
            peak, sums = take(sweep - 1)
            give(sweep, jnp.where(row8 == 0, peak, sums))

    y = lax.broadcasted_iota(jnp.int32, (rows, lanes), 0)
    z = lax.broadcasted_iota(jnp.int32, (rows, lanes), 1)
    y = place[1] * ly + jnp.where(y < ly + D, y, y - rows)
    z = place[2] * lz + jnp.where(z < lz + lz // 2, z, z - lanes)
    flat = jnp.where((y >= 0) & (y < ny) & (z >= 0) & (z < nz), 1.0, 0.0)

    def planar(v):
        a1, b1 = up(v, 1), down(v, 1)
        sz = a1 + b1
        sz2 = up(a1, 1) + down(b1, 1)
        vu, vd = up(v, 0), down(v, 0)
        near = sz + (vu + vd)
        far = sz2 + (up(vu, 0) + down(vd, 0))
        corner = up(sz, 0) + down(sz, 0)
        return (2.5 * v + 1.5 * near + FACE * corner + 0.5 * far, 1.5 * v + FACE * near + DIAGONAL * corner, 0.5 * v)

    h0, h1, h2 = planar(flat)

    def inside(i):
        i = place[0] * lx + i
        return jnp.where((i >= 0) & (i < nx), 1.0, 0.0)

    def stage_raw(t, _):
        rho = RHO[t]
        e = raw_strain([A[t, c] for c in range(3)], [A[t + 1, c] for c in range(3)])
        worked = sum(B[t, i] * e[i] for i in range(6))
        raw = JB[t] - (2.97 * 0.25) * (rho * rho) * worked
        i = t - D
        h = h0 * inside(i) + h1 * (inside(i - 1) + inside(i + 1)) + h2 * (inside(i - 2) + inside(i + 2))
        q = planar(jnp.where(rho > 0.0, raw / h, 0.0))
        for j in range(3):
            Q[t - (D - 2), j] = q[j][0:ly, 0:lz]
        return 0

    lax.fori_loop(D - 2, D + lx + 2, stage_raw, 0)
    peak, sums = take(2)
    for m in pending:
        m.drain()
    agg_out[0, 0] = jnp.max((peak + jnp.log(sums)) / power_scale)
    scale = jnp.exp(top - peak) / sums * float(nx * ny * nz)
    for x in range(lx):
        for c in range(3):
            adj_out[c, x] = A[D + x, c, 0:ly, 0:lz] * scale
        sens_out[x] = ((Q[x, 2] + Q[x + 1, 1]) + Q[x + 2, 0] + (Q[x + 3, 1] + Q[x + 4, 2])) * scale


def on_device(displacement, density):
    lx, ly, lz = density.shape
    slots = lax.axis_size("gx") + lax.axis_size("gy") + lax.axis_size("gz")
    group = lx + 2
    vmem = pl.BlockSpec(memory_space=pltpu.VMEM)
    X, R, L = lx + 2 * D, ly + 2 * D, 2 * lz
    f32 = jnp.float32
    shapes = [
        (X + 1, 3, ly + 3 * D, L), (X, R, L), (X, 6, R, L), (X, R, L), (X, R, L), (X, 6, R, L),
        (X, 3, R, L), (X, R, L), (X, R, L), (X, 3, R, L), (lx + 4, 3, ly, lz),
    ]
    dma = pltpu.SemaphoreType.DMA
    aggregate, adjoint, sens = pl.pallas_call(
        kernel,
        out_shape=(
            jax.ShapeDtypeStruct((1, 1), f32),
            jax.ShapeDtypeStruct((3, lx, ly, lz), f32),
            jax.ShapeDtypeStruct((lx, ly, lz), f32),
        ),
        in_specs=[vmem, vmem],
        out_specs=(pl.BlockSpec(memory_space=pltpu.SMEM), vmem, vmem),
        scratch_shapes=[
            pltpu.VMEM((4, 3 * group, R, lz), f32),
            pltpu.VMEM((4, 32, lz), f32),
            pltpu.VMEM((2, 4, R, lz), f32),
            pltpu.VMEM((32, lz), f32),
            pltpu.VMEM((2, 4, ly, lz), f32),
            dma((32,)), dma((32,)),
            pltpu.VMEM((slots, 8, lz), f32),
            dma((slots,)), dma((slots,)),
        ] + [pltpu.VMEM(s, f32) for s in shapes],
        compiler_params=pltpu.CompilerParams(has_side_effects=True, collective_id=0, vmem_limit_bytes=60 * 2**20),
    )(displacement, density)
    return aggregate[0, 0], adjoint, sens


def solution(mesh):
    return jax.shard_map(
        on_device,
        mesh=mesh,
        in_specs=(P(None, "gx", "gy", "gz"), P("gx", "gy", "gz")),
        out_specs=(P(), P(None, "gx", "gy", "gz"), P("gx", "gy", "gz")),
        check_vma=False,
    )
```

```python
import functools
import math

import jax
import jax.numpy as jnp
from jax import lax
from jax.experimental import pallas as pl
from jax.experimental.pallas import tpu as pltpu
from jax.sharding import PartitionSpec as P

ITERS = 6
lame = 0.3 / (1.3 * 0.4)
shear = 1.0 / 2.6
power_scale = 3.0
damping = 0.6
shift_term = 0.1
diag_factor = (lame + 3.0 * shear) / 16.0
FACE = 2.5 - math.sqrt(2.0)
DIAGONAL = 2.5 - math.sqrt(3.0)
MESH = pl.DeviceIdType.MESH
D = 8
C = 16


class Message:
    def __init__(self, sems, number, axis, step, src, dst, cond=None):
        index, count = lax.axis_index(axis), lax.axis_size(axis)
        self.args = (src, dst, sems[0].at[number], sems[1].at[number], axis, index, step)
        self.sends = (index + step >= 0) & (index + step < count)
        self.gets = (index - step >= 0) & (index - step < count)
        if cond is not None:
            self.sends, self.gets = self.sends & cond, self.gets & cond
        self.dst = dst

    def copy(self, sign):
        src, dst, ssem, rsem, axis, index, step = self.args
        return pltpu.make_async_remote_copy(
            src_ref=src, dst_ref=dst, send_sem=ssem, recv_sem=rsem,
            device_id={axis: index + sign * step}, device_id_type=MESH)

    def start(self):
        pl.when(self.sends)(lambda: self.copy(1).start())

    def clear(self):
        def zero():
            self.dst[...] = jnp.zeros(self.dst.shape, jnp.float32)

        pl.when(jnp.logical_not(self.gets))(zero)

    def arrive(self):
        pl.when(self.gets)(lambda: self.copy(-1).wait_recv())

    def drain(self):
        pl.when(self.sends)(lambda: self.copy(1).wait_send())


def gather(u_ref, rho_ref, ext, T, W, V, pack, ssem, rsem):
    lx, ly, lz = rho_ref.shape
    group = lx + 2
    iy, ny = lax.axis_index("gy"), lax.axis_size("gy")
    has_above, has_below = iy + 1 < ny, iy > 0
    own, upper, lower = pl.ds(0, ly), pl.ds(ly, D), pl.ds(ly + D, D)
    u3, r1, both = pl.ds(0, 3), pl.ds(3, 1), pl.ds(0, 2)
    numbers = iter(range(64))

    def msg(axis, step, src, dst, cond=None):
        return Message((ssem, rsem), next(numbers), axis, step, src, dst, cond)

    def body(g):
        return pl.ds(g * group + 2, lx)

    def whole(g):
        return pl.ds(g * group, group)

    def halo(g):
        return pl.ds(g * group, 2)

    z = [msg("gz", -1, pack.at[0], ext.at[:, 0, own]), msg("gz", 1, pack.at[1], ext.at[:, 1, own])]
    y, x = [], []
    for step, rows, to in ((1, pl.ds(ly - D, D), lower), (-1, pl.ds(0, D), upper)):
        y.append(msg("gy", step, u_ref.at[:, :, rows], ext.at[u3, body(0), to]))
        y.append(msg("gy", step, rho_ref.at[:, rows], ext.at[3, body(0), to]))
    for step, g in ((1, 1), (-1, 2)):
        x.append(msg("gx", step, u_ref, ext.at[u3, body(g), own]))
        x.append(msg("gx", step, rho_ref, ext.at[3, body(g), own]))
    y2, x2, x3 = [], [], []
    for step, rows, to in ((1, pl.ds(ly - D, D), lower), (-1, pl.ds(0, D), upper)):
        y2.append(msg("gy", step, ext.at[:, both, rows], ext.at[:, both, to]))
    y2.append(msg("gy", -1, V, T.at[0]))
    for step, g in ((1, 1), (-1, 2)):
        x2.append(msg("gx", step, ext.at[:, halo(0), own], ext.at[:, halo(g), own]))
        x3.append(msg("gx", step, ext.at[:, whole(0), upper], ext.at[:, whole(g), upper], has_above))
        x3.append(msg("gx", step, ext.at[:, whole(0), lower], ext.at[:, whole(g), lower], has_below))
        x3.append(msg("gx", step, T.at[0], T.at[g], has_above))
    x3.append(msg("gx", -2, T.at[0], T.at[3], has_above))
    x3.append(msg("gx", -2, W.at[0], W.at[1]))
    every = z + y + x + y2 + x2 + x3

    for m in y + x:
        m.start()
    lane = lax.broadcasted_iota(jnp.int32, (ly, lz), 1)
    for c in range(4):
        first = jnp.zeros((ly, lz), jnp.float32)
        last = first
        for i in range(lx):
            tile = u_ref[c, i] if c < 3 else rho_ref[i]
            here = (lane >= C * i) & (lane < C * i + C)
            first = jnp.where(here, pltpu.roll(tile, C * i, 1) if i else tile, first)
            last = jnp.where(here, pltpu.roll(tile, (C * i + C) % lz, 1), last)
        pack[0, c] = first
        pack[1, c] = last
    for m in z:
        m.start()
    for m in every:
        m.clear()
    V[...] = jnp.zeros(V.shape, jnp.float32)
    for c in range(3):
        for i in range(lx):
            k = c * group + 2 + i
            V[k:k + 1] = u_ref[c, i, D:D + 1]
            ext[c, 2 + i, 0:ly] = u_ref[c, i]
    for i in range(lx):
        ext[3, 2 + i, 0:ly] = rho_ref[i]
    for m in z:
        m.arrive()
    for m in x2:
        m.start()
    for m in y2[:2]:
        m.start()
    for c in range(3):
        for i in range(2):
            k = c * group + i
            V[k:k + 1] = ext[c, i, D:D + 1]
    y2[2].start()
    for m in y + y2:
        m.arrive()
    for m in x3[:-1]:
        m.start()
    wide = lax.broadcasted_iota(jnp.int32, (ly + 2 * D, lz), 1)
    side = jnp.zeros((ly + 2 * D, lz), jnp.float32)
    for c in range(3):
        W[0, c] = ext[c, 2]
        for i in range(2):
            at = 2 * C * c + C * i
            tile = ext[c, i]
            tile = pltpu.roll(tile, at, 1) if at else tile
            side = jnp.where((wide >= at) & (wide < at + C), tile, side)
    W[0, 3] = side
    x3[-1].start()
    lower_side = x[:2] + x2[:1] + x3[:3]
    upper_side = x[2:] + x2[1:] + x3[3:6]
    return every, (lower_side, upper_side, x3[6:])


def up(v, axis):
    return pltpu.roll(v, v.shape[axis] - 1, axis)


def down(v, axis):
    return pltpu.roll(v, 1, axis)


def raw_strain(low, high):
    g = []
    for c in range(3):
        s = low[c] + high[c]
        d = high[c] - low[c]
        s1, d1 = up(s, 1), up(d, 1)
        za, zd, xd = s + s1, s1 - s, d + d1
        g.append((xd + up(xd, 0), up(za, 0) - za, zd + up(zd, 0)))
    return (g[0][0], g[1][1], g[2][2], g[1][0] + g[0][1], g[2][1] + g[1][2], g[0][2] + g[2][0])


def cmul(t):
    tr = lame * (t[0] + t[1] + t[2])
    return [tr + (2.0 * shear) * t[i] for i in range(3)] + [shear * t[i] for i in range(3, 6)]


ROWS = ((0, 3, 5), (3, 1, 4), (5, 4, 2))


def gather_forces(a, b):
    out = []
    for c in range(3):
        i, j, k = ROWS[c]
        x = a[i] - b[i]
        y = a[j] + b[j]
        z = a[k] + b[k]
        w = down(x + y, 0) + (x - y)
        v = down(z, 0) + z
        out.append(down(w + v, 1) + (w - v))
    return out


def kernel(u_ref, rho_ref, agg_out, adj_out, sens_out, ext, T, W, V, pack, ssem, rsem, ST, gsem, hsem, U, RHO, B, VM, JB, S, LOAD, DM, K16, A, Q, EM):
    lx, ly, lz = sens_out.shape
    axes = ("gx", "gy", "gz")
    barrier = pltpu.get_barrier_semaphore()
    friends = 0
    for axis in axes:
        index, count = lax.axis_index(axis), lax.axis_size(axis)
        friends += count - 1
        for step in range(1, count):
            pl.semaphore_signal(barrier, inc=1, device_id={axis: (index + step) % count}, device_id_type=MESH)
    pl.semaphore_wait(barrier, friends)
    place = [lax.axis_index(a) for a in axes]
    counts = [lax.axis_size(a) for a in axes]
    nx, ny, nz = counts[0] * lx, counts[1] * ly, counts[2] * lz
    group = lx + 2
    pending, arrivals = gather(u_ref, rho_ref, ext, T, W, V, pack, ssem, rsem)
    X = lx + 2 * D
    rows, lanes = ly + 2 * D, 2 * lz
    wide = (ly + 3 * D, lz)
    lane = lax.broadcasted_iota(jnp.int32, wide, 1)

    def tall(v, row):
        return jnp.concatenate([v[0:ly + D], jnp.broadcast_to(row, (D, lz)), v[ly + D:rows]], axis=0)

    def turn(v, amount):
        return pltpu.roll(v, amount % lz, 1) if amount % lz else v

    def unpack(t):
        g, xi = divmod(t, lx)
        base = (group, 0, 2 * group, 0)[g]
        tg = (1, 0, 2, 3)[g]
        for c in range(3):
            k = c * group
            if t < X:
                main, above, below = ext[c, base + 2 + xi], ext[c, base], ext[c, base + 1]
                above, below = turn(above, -C * xi), turn(below, -C - C * xi)
            else:
                main, side = W[1, c], W[1, 3]
                above, below = turn(side, -2 * C * c), turn(side, -2 * C * c - 2 * C)
            above = tall(above, turn(T[tg, k:k + 1], -C * xi))
            below = tall(below, turn(T[tg, k + 1:k + 2], -C - C * xi))
            U[t, c, :, 0:lz] = tall(main, T[tg, k + 2 + xi:k + 3 + xi])
            U[t, c, :, lz:lanes] = jnp.where(lane < D + 1, above, jnp.where(lane >= lz - D, below, 0.0))
        if t < X:
            above, below = turn(ext[3, base], -C * xi), turn(ext[3, base + 1], -C - C * xi)
            thin = lane[0:rows]
            RHO[t, :, 0:lz] = ext[3, base + 2 + xi]
            RHO[t, :, lz:lanes] = jnp.where(thin < D, above, jnp.where(thin >= lz - D, below, 0.0))

    def cut(v):
        return jnp.concatenate([v[0:ly + D], v[ly + 2 * D:ly + 3 * D]], axis=0)

    def stage_one(t, best):
        low = [U[t, c] for c in range(3)]
        high = [U[t + 1, c] for c in range(3)]
        b = cmul([cut(0.25 * e) for e in raw_strain(low, high)])
        j = (b[0] * b[0] + b[1] * b[1] + b[2] * b[2] - b[0] * b[1] - b[1] * b[2] - b[2] * b[0]
             + 3.0 * (b[3] * b[3] + b[4] * b[4] + b[5] * b[5]))
        rho = RHO[t]
        vm = jnp.sqrt(rho * j + 1.0)
        for i in range(6):
            B[t, i] = b[i]
        JB[t] = j
        VM[t] = vm
        K16[t] = jnp.where(rho > 0.0, (0.01 + 0.99 * (rho * rho * rho)) * (0.125 * shear), 0.0)
        return jnp.maximum(best, vm)

    best = jnp.ones((rows, lanes), jnp.float32)
    for t in range(D, D + lx):
        unpack(t)
    best = lax.fori_loop(D, D + lx - 1, stage_one, best)
    for m in arrivals[0]:
        m.arrive()
    for t in range(D):
        unpack(t)
    best = lax.fori_loop(0, D, stage_one, best, unroll=2)
    for m in arrivals[1]:
        m.arrive()
    for t in range(D + lx, X):
        unpack(t)
    best = lax.fori_loop(D + lx - 1, X - 1, stage_one, best, unroll=2)
    for m in arrivals[2]:
        m.arrive()
    unpack(X)
    best = stage_one(X - 1, best)
    top = power_scale * jnp.max(best)

    def stage_two(t, _):
        vm = VM[t]
        weight = jnp.exp(power_scale * vm - top)
        factor = weight / (2.0 * vm)
        f = factor * RHO[t] * (0.5 * shear)
        b = [B[t, i] for i in range(6)]
        tr = b[0] + b[1] + b[2]
        for i in range(3):
            S[t, i] = f * (3.0 * b[i] - tr)
        for i in range(3, 6):
            S[t, i] = (3.0 * f) * b[i]
        JB[t] = factor * JB[t]
        VM[t] = weight
        return 0

    lax.fori_loop(0, X, stage_two, 0, unroll=2)
    total = jnp.sum(VM[D:D + lx, 0:ly, 0:lz])
    row8 = lax.broadcasted_iota(jnp.int32, (8, lz), 0)
    starts = (0, counts[0], counts[0] + counts[1])
    state = jnp.where(row8 == 0, top, total)

    def partner(p, k, sign):
        index, count = place[p], counts[p]
        other = (index + sign * k) % count if sign > 0 else (index - k + count) % count
        slot = starts[p] + (index if sign > 0 else other)
        return pltpu.make_async_remote_copy(
            src_ref=ST.at[slot], dst_ref=ST.at[slot],
            send_sem=gsem.at[starts[p] + k], recv_sem=hsem.at[starts[p] + k],
            device_id={axes[p]: other}, device_id_type=MESH)

    def give(p, value):
        ST[starts[p] + place[p]] = value
        for k in range(1, counts[p]):
            partner(p, k, 1).start()

    def take(p):
        for k in range(1, counts[p]):
            partner(p, k, -1).wait_recv()
        for k in range(1, counts[p]):
            partner(p, k, 1).wait_send()
        tiles = ST[starts[p]:starts[p] + counts[p]]
        tops, totals = tiles[:, 0, :], tiles[:, 1, :]
        peak = jnp.max(tops, axis=0, keepdims=True)
        sums = jnp.sum(totals * jnp.exp(tops - peak), axis=0, keepdims=True)
        return peak, sums

    give(0, state)

    def stage_load(t, _):
        f = gather_forces([S[t - 1, i] for i in range(6)], [S[t, i] for i in range(6)])
        k = K16[t - 1] + K16[t]
        k = k + down(k, 0)
        k = k + down(k, 1)
        dm = jnp.where(RHO[t] > 0.0, damping / ((8.0 * diag_factor / shear) * k + shift_term), 0.0)
        DM[t] = dm
        EM[t] = 1.0 - shift_term * dm
        for c in range(3):
            LOAD[t, c] = dm * f[c]
            A[t, c] = dm * f[c]
        return 0

    stage_load(1, 0)
    lax.fori_loop(2, X, stage_load, 0, unroll=2)

    for sweep in range(1, ITERS):
        def stress(t, _):
            n = raw_strain([A[t, c] for c in range(3)], [A[t + 1, c] for c in range(3)])
            k = K16[t]
            half = 0.5 * k
            tr = (lame / (2.0 * shear)) * (n[0] + n[1] + n[2])
            for i in range(3):
                S[t, i] = k * (n[i] + tr)
            for i in range(3, 6):
                S[t, i] = half * n[i]
            return 0

        def update(t, _):
            f = gather_forces([S[t - 1, i] for i in range(6)], [S[t, i] for i in range(6)])
            dm, keep = DM[t], EM[t]
            for c in range(3):
                A[t, c] = (keep * A[t, c] + LOAD[t, c]) - dm * f[c]
            return 0

        lax.fori_loop(sweep, X - sweep, stress, 0, unroll=2)
        lax.fori_loop(sweep + 1, X - sweep + 1, update, 0, unroll=2)
        if sweep <= 2:
            peak, sums = take(sweep - 1)
            give(sweep, jnp.where(row8 == 0, peak, sums))

    y = lax.broadcasted_iota(jnp.int32, (rows, lanes), 0)
    z = lax.broadcasted_iota(jnp.int32, (rows, lanes), 1)
    y = place[1] * ly + jnp.where(y < ly + D, y, y - rows)
    z = place[2] * lz + jnp.where(z < lz + lz // 2, z, z - lanes)
    flat = jnp.where((y >= 0) & (y < ny) & (z >= 0) & (z < nz), 1.0, 0.0)

    def planar(v, tall=None, wide=None):
        own = (slice(0, tall), slice(0, wide))
        a1, b1 = up(v, 1), down(v, 1)
        sz = (a1 + b1)[:, 0:wide]
        sz2 = up(a1, 1)[own] + down(b1, 1)[own]
        n = v[:, 0:wide]
        vu, vd = up(n, 0), down(n, 0)
        near = sz[0:tall] + (vu + vd)[0:tall]
        far = sz2 + (up(vu, 0) + down(vd, 0))[0:tall]
        corner = (up(sz, 0) + down(sz, 0))[0:tall]
        v = v[own]
        return (2.5 * v + 1.5 * near + FACE * corner + 0.5 * far, 1.5 * v + FACE * near + DIAGONAL * corner, 0.5 * v)

    h0, h1, h2 = planar(flat)

    def inside(i):
        i = place[0] * lx + i
        return jnp.where((i >= 0) & (i < nx), 1.0, 0.0)

    def stage_raw(t, _):
        rho = RHO[t]
        e = raw_strain([A[t, c] for c in range(3)], [A[t + 1, c] for c in range(3)])
        worked = sum(B[t, i] * e[i] for i in range(6))
        raw = JB[t] - (2.97 * 0.25) * (rho * rho) * worked
        i = t - D
        h = h0 * inside(i) + h1 * (inside(i - 1) + inside(i + 1)) + h2 * (inside(i - 2) + inside(i + 2))
        q = planar(jnp.where(rho > 0.0, raw / h, 0.0), ly, lz)
        for j in range(3):
            Q[t - (D - 2), j] = q[j]
        return 0

    lax.fori_loop(D - 2, D + lx + 2, stage_raw, 0, unroll=2)
    peak, sums = take(2)
    for m in pending:
        m.drain()
    agg_out[0, 0] = jnp.max((peak + jnp.log(sums)) / power_scale)
    scale = jnp.exp(top - peak) / sums * float(nx * ny * nz)
    for x in range(lx):
        for c in range(3):
            adj_out[c, x] = A[D + x, c, 0:ly, 0:lz] * scale
        sens_out[x] = ((Q[x, 2] + Q[x + 1, 1]) + Q[x + 2, 0] + (Q[x + 3, 1] + Q[x + 4, 2])) * scale


def on_device(displacement, density):
    lx, ly, lz = density.shape
    slots = lax.axis_size("gx") + lax.axis_size("gy") + lax.axis_size("gz")
    group = lx + 2
    vmem = pl.BlockSpec(memory_space=pltpu.VMEM)
    X, R, L = lx + 2 * D, ly + 2 * D, 2 * lz
    f32 = jnp.float32
    shapes = [
        (X + 1, 3, ly + 3 * D, L), (X, R, L), (X, 6, R, L), (X, R, L), (X, R, L), (X, 6, R, L),
        (X, 3, R, L), (X, R, L), (X, R, L), (X, 3, R, L), (lx + 4, 3, ly, lz), (X, R, L),
    ]
    dma = pltpu.SemaphoreType.DMA
    aggregate, adjoint, sens = pl.pallas_call(
        kernel,
        out_shape=(
            jax.ShapeDtypeStruct((1, 1), f32),
            jax.ShapeDtypeStruct((3, lx, ly, lz), f32),
            jax.ShapeDtypeStruct((lx, ly, lz), f32),
        ),
        in_specs=[vmem, vmem],
        out_specs=(pl.BlockSpec(memory_space=pltpu.SMEM), vmem, vmem),
        scratch_shapes=[
            pltpu.VMEM((4, 3 * group, R, lz), f32),
            pltpu.VMEM((4, 32, lz), f32),
            pltpu.VMEM((2, 4, R, lz), f32),
            pltpu.VMEM((32, lz), f32),
            pltpu.VMEM((2, 4, ly, lz), f32),
            dma((32,)), dma((32,)),
            pltpu.VMEM((slots, 8, lz), f32),
            dma((slots,)), dma((slots,)),
        ] + [pltpu.VMEM(s, f32) for s in shapes],
        compiler_params=pltpu.CompilerParams(has_side_effects=True, collective_id=0, vmem_limit_bytes=60 * 2**20),
    )(displacement, density)
    return aggregate[0, 0], adjoint, sens


def solution(mesh):
    return jax.shard_map(
        on_device,
        mesh=mesh,
        in_specs=(P(None, "gx", "gy", "gz"), P("gx", "gy", "gz")),
        out_specs=(P(), P(None, "gx", "gy", "gz"), P("gx", "gy", "gz")),
        check_vma=False,
    )
```
